32 devices in a mesh: row: 4 (over y, x), col: 8 (over z, core).
Axes of the slice: x: 2, y: 2, z: 4, core: 2. Of those that a mesh axis runs over, the one named last changes fastest.
Arguments:
- gate_pre: bfloat16 [1024, 26624], P('col', 'row'), may hold values from -6 to 6
- up_pre: bfloat16 [1024, 26624], P('col', 'row'), may hold values from -6 to 6
- residual: bfloat16 [1024, 16384], P('row', 'col'), may hold values from -6 to 6
- base_weight: bfloat16 [26624, 16384], P('row', 'col'), may hold values from -0.0390625 to 0.0390625
- perturb: bfloat16 [26624, 16384], P('row', 'col'), may hold values from -0.0390625 to 0.0390625
- exponents: int32 [208, 16384], P('row', 'col'), may hold values from -2 to 1
Outputs:
- plus_out: bfloat16 [1024, 16384], P('row', 'col')
- minus_out: bfloat16 [1024, 16384], P('row', 'col')
The draws below stay inside these ranges and needn't reach their ends.
All inputs are finite; a program needn't handle non-finite values.
Results may differ from the reference program's by a relative error of at most 0.004.
Values may be sent and summed in bfloat16 or wider, within the bound.
No kernel may reach another device: no remote copies, remote signals or barrier semaphores. Data moves between devices by JAX's collectives and lax.ppermute only.
A program may use at most 192 MiB of HBM per device.

```python
import jax
import jax.numpy as jnp
from jax import lax

D = 16384
FF = 26624
GROUP = 128
TOKENS = 1024
N_COL = 8


def touch_ends(array, own_key, smallest, high):
    dims = array.shape
    spot = [jax.random.randint(jax.random.fold_in(own_key, axis), (), 0, dims[axis]) for axis in range(len(dims))]
    array = array.at[tuple(spot)].set(smallest)
    longest = dims.index(max(dims))
    spot[longest] = (spot[longest] + 1) % dims[longest]
    return array.at[tuple(spot)].set(high)


def level_of(rng, extent, shards, low, high):
    gain, own = 1.0, jax.random.fold_in(rng, 6)
    for position, blocks in shards:
        steps = jnp.exp(jax.random.uniform(jax.random.fold_in(own, position), (blocks,), jnp.float32, low / len(shards), high / len(shards)))
        gain = gain * jnp.repeat(steps, extent[position] // blocks).reshape([-1 if axis == position else 1 for axis in range(len(extent))])
    return gain


def bell_draw(key, shape, spread, reach, split=(), held_as=jnp.bfloat16):
    array = spread * jax.random.normal(key, shape, jnp.float32)
    if split:
        array = array * level_of(key, shape, split, -0.22, 0.18)
    return jnp.clip(array, -reach, reach).astype(held_as)


def setup_inputs(seed: int = 0) -> dict:
    keys = jax.random.split(jax.random.key(seed), 7)
    return {
        "gate_pre": bell_draw(keys[0], (TOKENS, FF), 1.0, 6.0, ((0, 8), (1, 4))),
        "up_pre": bell_draw(keys[1], (TOKENS, FF), 1.0, 6.0, ((0, 8), (1, 4))),
        "residual": bell_draw(keys[2], (TOKENS, D), 1.0, 6.0, ((0, 4), (1, 8))),
        "base_weight": bell_draw(keys[3], (FF, D), FF ** -0.5, 0.0390625, ((0, 4), (1, 8))),
        "perturb": bell_draw(keys[4], (FF, D), FF ** -0.5, 0.0390625, ((0, 4), (1, 8))),
        "exponents": touch_ends(jax.random.randint(keys[5], (FF // GROUP, D), -2, 2), jax.random.fold_in(keys[5], 1), -2, 1).astype(jnp.int32),
    }


step_size = 0.25


def reference(gate_pre, up_pre, residual, base_weight, perturb, exponents):
    hidden = (jax.nn.silu(gate_pre.astype(jnp.float32)) * up_pre.astype(jnp.float32)).astype(jnp.bfloat16)
    columns = D // N_COL

    def column_block(block_index):
        offset = (block_index * columns).astype(jnp.int32)
        weight_block = lax.dynamic_slice_in_dim(base_weight, offset, columns, 1).astype(jnp.float32)
        direction = lax.dynamic_slice_in_dim(perturb, offset, columns, 1).astype(jnp.float32)
        powers = lax.dynamic_slice_in_dim(exponents, offset, columns, 1)
        factor = jnp.repeat(jnp.exp2(powers.astype(jnp.float32)), GROUP, axis=0)
        shift = step_size * factor * direction
        plus_weight = (weight_block + shift).astype(jnp.bfloat16)
        minus_weight = (weight_block - shift).astype(jnp.bfloat16)
        stream = lax.dynamic_slice_in_dim(residual, offset, columns, 1).astype(jnp.float32)
        plus_part = (stream + jnp.dot(hidden, plus_weight, preferred_element_type=jnp.float32)).astype(jnp.bfloat16)
        minus_part = (stream + jnp.dot(hidden, minus_weight, preferred_element_type=jnp.float32)).astype(jnp.bfloat16)
        return plus_part, minus_part

    plus_blocks, minus_blocks = lax.map(column_block, jnp.arange(N_COL, dtype=jnp.int32))
    plus_out = jnp.transpose(plus_blocks, (1, 0, 2)).reshape(TOKENS, D)
    minus_out = jnp.transpose(minus_blocks, (1, 0, 2)).reshape(TOKENS, D)
    return plus_out, minus_out
```

```python
import functools

import jax
import jax.numpy as jnp
from jax import lax
from jax.experimental import pallas as pl
from jax.experimental.pallas import tpu as pltpu
from jax.sharding import PartitionSpec as P


step_size = 0.25


HBM = pltpu.MemorySpace.HBM
VMEM = pltpu.MemorySpace.VMEM

VMEM_BYTES = 67_043_328


def beside(weight_bytes):
    return pltpu.CompilerParams(vmem_limit_bytes=VMEM_BYTES - 2 * weight_bytes)


def in_hbm(*arrays):
    return tuple(pltpu.with_memory_space_constraint(array, HBM) for array in arrays)


LOADS = 2

PIECES = ((2, 1, False), (2, 1, False), (2, 1, False), (2, 2, False))


def swiglu_kernel(starts, gate_ref, up_ref, *hidden_refs):
    for start, hidden_ref in zip(starts, hidden_refs):
        rows = pl.ds(start, hidden_ref.shape[0])
        gate = gate_ref[rows].astype(jnp.float32)
        up = up_ref[rows].astype(jnp.float32)
        hidden_ref[...] = (gate / (1.0 + jnp.exp(-gate)) * up).astype(hidden_ref.dtype)


def swiglu(gate_pre, up_pre, start, counts, limit):
    width = gate_pre.shape[1]
    rows = sum(counts)
    whole = start % rows != 0
    block = width // 2
    held = gate_pre.shape[0] if whole else rows
    spec = pl.BlockSpec((held, block), lambda i: (0 if whole else start // rows, i))
    starts = [(start if whole else 0) + sum(counts[:k]) for k in range(len(counts))]
    return pl.pallas_call(
        functools.partial(swiglu_kernel, starts),
        grid=(2,),
        in_specs=[spec, spec],
        out_specs=[pl.BlockSpec((count, block), lambda i: (0, i)) for count in counts],
        out_shape=[pltpu.HBM((count, width), jnp.bfloat16) for count in counts],
        compiler_params=limit,
        cost_estimate=pl.CostEstimate(
            flops=20 * rows * width, bytes_accessed=6 * rows * width, transcendentals=2 * rows * width
        ),
        name="swiglu",
    )(*in_hbm(gate_pre, up_pre))


def perturb_kernel(part, base_ref, perturb_ref, exp_ref, *refs):
    plus, minus, exps, sems, exp_sem = refs[-5:]
    depth = plus.shape[0]
    group = base_ref.shape[0] // exps.shape[0]
    groups = depth // group
    chunks = sems.shape[1]
    per_chunk = groups // chunks
    copies = [pltpu.make_async_copy(exp_ref, exps, exp_sem)]
    for k in range(chunks):
        rows = pl.ds(k * per_chunk * group, per_chunk * group)
        there = pl.ds(part * depth + k * per_chunk * group, per_chunk * group)
        copies.append(pltpu.make_async_copy(base_ref.at[there], plus.at[rows], sems.at[0, k]))
        copies.append(pltpu.make_async_copy(perturb_ref.at[there], minus.at[rows], sems.at[1, k]))
    for copy in copies:
        copy.start()
    copies[0].wait()
    for k in range(chunks):
        copies[1 + 2 * k].wait()
        copies[2 + 2 * k].wait()

        @pl.loop(k * per_chunk, (k + 1) * per_chunk)
        def _(g):
            rows = pl.ds(pl.multiple_of(g * group, group), group)
            factor = (step_size * jnp.exp2(exps[pl.ds(part * groups + g, 1), :].astype(jnp.float32))).astype(
                plus.dtype
            )
            shift = minus[rows] * factor
            base = plus[rows]
            plus[rows] = base + shift
            minus[rows] = base - shift


def place_kernel(hidden_ref, *outs):
    del hidden_ref, outs


def in_vmem(arrays):
    return tuple(pltpu.with_memory_space_constraint(array, VMEM) for array in arrays)


def places(hidden, base, limit):
    return pl.pallas_call(
        place_kernel,
        in_specs=[pl.BlockSpec(memory_space=HBM)],
        out_specs=[pl.BlockSpec(memory_space=VMEM)] * (2 * LOADS),
        out_shape=[pltpu.VMEM((base.shape[0] // LOADS, base.shape[1]), base.dtype)] * (2 * LOADS),
        compiler_params=limit,
        name="places",
    )(*in_hbm(hidden))


def perturbed(base, perturb, exponents, room, part, limit):
    depth = base.shape[0] // LOADS
    groups = exponents.shape[0] // LOADS
    chunks = 13 if groups % 13 == 0 else 1
    return pl.pallas_call(
        functools.partial(perturb_kernel, part),
        in_specs=[pl.BlockSpec(memory_space=HBM)] * 3 + [pl.BlockSpec(memory_space=VMEM)] * 2,
        out_specs=[pl.BlockSpec(memory_space=VMEM)] * 2,
        out_shape=[pltpu.VMEM((depth, base.shape[1]), base.dtype)] * 2,
        input_output_aliases={3: 0, 4: 1},
        scratch_shapes=[
            pltpu.VMEM(exponents.shape, exponents.dtype),
            pltpu.SemaphoreType.DMA((2, chunks)),
            pltpu.SemaphoreType.DMA,
        ],
        compiler_params=limit,
        cost_estimate=pl.CostEstimate(
            flops=10_000_000_000, bytes_accessed=4 * base.size // LOADS, transcendentals=0
        ),
        name="perturbed",
    )(*in_hbm(base, perturb, exponents), *in_vmem(room))


def project_kernel(chips, rows, first, block, *refs):
    items = refs[: 2 * chips]
    weights = refs[2 * chips : 2 * chips + 2 * LOADS]
    outs = refs[2 * chips + 2 * LOADS : 3 * chips + 2 * LOADS]
    hidden, sem = refs[3 * chips + 2 * LOADS :]
    col = lax.axis_index("col")
    chip, core = col // 2, lax.rem(col, 2)
    mix = chip ^ lax.axis_index("row")

    @pl.when(pl.program_id(0) == 0)
    def _():
        copies = []
        for index in range(chips):
            for swapped in range(2):
                place = (index ^ mix) * 2 + (core ^ swapped)
                copies.append(
                    pltpu.make_async_copy(
                        items[2 * index + swapped],
                        hidden.at[pl.ds(pl.multiple_of(place * rows, rows), rows)],
                        sem.at[2 * index + swapped],
                    )
                )
        for copy in copies:
            copy.start()
        for copy in copies:
            copy.wait()

    columns = pl.ds(pl.multiple_of((first + pl.program_id(0)) * block, block), block)
    depth = weights[0].shape[0]
    for which in range(2):
        total = sum(
            jnp.dot(
                hidden[:, k * depth : (k + 1) * depth],
                weights[2 * k + which][:, columns],
                preferred_element_type=jnp.float32,
            )
            for k in range(LOADS)
        )
        for slot, out in enumerate(outs):
            out[which] = total[slot * 2 * rows : (slot + 1) * 2 * rows].astype(out.dtype)


def project(items, weights, part, parts, limit, block=512):
    chips = len(items) // 2
    rows, depth = items[0].shape
    width = weights[0].shape[1] // parts
    block = min(block, width)
    tokens = 2 * chips * rows
    return pl.pallas_call(
        functools.partial(project_kernel, chips, rows, part * (width // block), block),
        grid=(width // block,),
        in_specs=[pl.BlockSpec(memory_space=HBM)] * (2 * chips) + [pl.BlockSpec(memory_space=VMEM)] * (2 * LOADS),
        out_specs=[pl.BlockSpec((2, 2 * rows, block), lambda i: (0, 0, i))] * chips,
        out_shape=[
            pltpu.HBM((2, 2 * rows, width), jnp.float32 if slot == 0 else jnp.bfloat16)
            for slot in range(chips)
        ],
        scratch_shapes=[
            pltpu.VMEM((tokens, depth), jnp.bfloat16),
            pltpu.SemaphoreType.DMA((2 * chips,)),
        ],
        compiler_params=limit,
        cost_estimate=pl.CostEstimate(
            flops=4 * tokens * depth * width, bytes_accessed=2 * tokens * depth, transcendentals=0
        ),
        name="project",
    )(*in_hbm(*items), *in_vmem(weights))


def finish_kernel(spans, peers, *refs):
    count = len(spans) * (1 + peers)
    residual_ref = refs[count]
    plus_ref, minus_ref = refs[-2:]
    half, held, width = residual_ref.shape
    for which, out in enumerate((plus_ref, minus_ref)):
        for k, (start, rows) in enumerate(spans):
            total = refs[k * (1 + peers)][which]
            for other in refs[k * (1 + peers) + 1 : (k + 1) * (1 + peers)]:
                total = total + other[which].astype(jnp.float32)
            place = pl.ds(start, rows)
            stream = residual_ref[:, place].astype(jnp.float32)
            out[:, place] = (stream + total.reshape(half, rows, width)).astype(out.dtype)
        covered = sum(rows for _, rows in spans)
        if covered < held:
            out[:, covered:] = residual_ref[:, covered:]


def finish(sums, residual, start, counts, part, parts, earlier, limit, block):
    half, held, features = residual.shape
    peers = len(sums[0]) - 1
    width = features // parts
    block = min(block, width)
    first = part * (width // block)
    rows = held if not earlier else sum(counts)
    kept = pl.BlockSpec((half, rows, block), lambda i: (0, start // rows, first + i))
    shape = pltpu.HBM(residual.shape, residual.dtype)
    spans = tuple((sum(counts[:k]), count) for k, count in enumerate(counts))
    arrays = [array for group in sums for array in group]
    return pl.pallas_call(
        functools.partial(finish_kernel, spans, peers),
        grid=(width // block,),
        in_specs=[
            pl.BlockSpec((2, half * count, block), lambda i: (0, 0, i)) for count in counts for _ in range(1 + peers)
        ]
        + [kept]
        + [pl.BlockSpec(memory_space=HBM)] * len(earlier),
        out_specs=[kept, kept],
        out_shape=[shape, shape],
        input_output_aliases={len(arrays) + 1 + i: i for i in range(len(earlier))},
        compiler_params=limit,
        cost_estimate=pl.CostEstimate(
            flops=10 * half * rows * width, bytes_accessed=30 * half * rows * width, transcendentals=0
        ),
        name="finish",
    )(*(arrays if earlier else in_hbm(*arrays)), *in_hbm(residual, *earlier))


def lowest(mask):
    return mask & -mask


def on_device(chips, row_count, gate_pre, up_pre, residual, base_weight, perturb, exponents):
    tokens = gate_pre.shape[0]
    halves = residual.reshape(2, tokens, residual.shape[1])

    to_chip = lambda array, bits: lax.ppermute(
        array, "col", [(c, c ^ (2 * bits)) for c in range(2 * chips)]
    )
    to_core = lambda array: lax.ppermute(array, "col", [(c, c ^ 1) for c in range(2 * chips)])
    to_row = lambda array, bits: lax.ppermute(array, "row", [(r, r ^ bits) for r in range(row_count)])

    limit = beside(base_weight.size * base_weight.dtype.itemsize)
    room = places(gate_pre, base_weight, limit)
    weights = ()
    for part in range(LOADS):
        weights += tuple(perturbed(base_weight, perturb, exponents, room[2 * part : 2 * part + 2], part, limit))
    counts = [tokens * share // 8 for share, _, _ in PIECES]
    first_hidden = list(swiglu(gate_pre, up_pre, 0, counts[:1], limit))
    first_hidden += swiglu(gate_pre, up_pre, counts[0], counts[1:], limit)
    sums = []
    for piece, (_, parts, straight) in enumerate(PIECES):
        items = [first_hidden[piece]]
        for mask in range(1, chips):
            bits = mask if straight else lowest(mask)
            items.append(to_chip(items[mask ^ bits], bits))
        held = []
        for item in items:
            held += [item, to_core(item)]
        for part in range(parts):
            own, *sent = project(held, weights, part, parts, limit)
            others = [to_row(array, k + 1) for k, array in enumerate(sent)]
            sums.append((own, *others))
    last = len(PIECES) - 1
    outs = finish(sums[:last], halves, 0, counts[:last], 0, 1, (), limit, 512)
    for part in range(PIECES[last][1]):
        outs = finish(
            sums[last + part : last + part + 1], halves, sum(counts[:last]), counts[last:],
            part, PIECES[last][1], outs, limit, 1024,
        )
    return tuple(out.reshape(residual.shape) for out in outs)


def solution(mesh):
    row_count = mesh.shape["row"]
    chips = mesh.shape["col"] // 2
    assert row_count == chips and chips & (chips - 1) == 0
    return jax.shard_map(
        functools.partial(on_device, chips, row_count),
        mesh=mesh,
        in_specs=(
            P("col", "row"),
            P("col", "row"),
            P("row", "col"),
            P("row", "col"),
            P("row", "col"),
            P("row", "col"),
        ),
        out_specs=(P("row", "col"), P("row", "col")),
        check_vma=False,
    )
```
